32 devices in a mesh: row: 4 (over y, x), col: 8 (over z, core).
Axes of the slice: x: 2, y: 2, z: 4, core: 2. Of those that a mesh axis runs over, the one named last changes fastest.
Arguments:
- trail_u: float32 [2, 4, 8, 64, 2048], P(None, 'row', 'col'), may hold values from -6 to 6
- trail_v: float32 [2, 4, 8, 64, 2048], P(None, 'row', 'col'), may hold values from -0.75 to 0.75
- ranks: int32 [2, 4, 8], P(None, 'row', 'col'), may hold values from 16 to 64
- panel_u: float32 [2, 4, 64, 2048], P(None, 'row', None, 'col'), may hold values from -6 to 6
- panel_v: float32 [2, 4, 64, 2048], P(None, 'row', None, 'col'), may hold values from -0.125 to 0.125
- locations: float32 [2, 4, 2, 2048], P(None, 'row', None, 'col'), may hold values from 0 to 1
- pend_locs: float32 [2, 2048], P(None, 'col'), may hold values from 0 to 1
- sketch: float32 [64, 2048], replicated, may hold values from -0.125 to 0.125
Outputs:
- trail_y: float32 [2, 4, 8, 64, 2048], P(None, 'row', 'col')
- trail_z: float32 [2, 4, 8, 64, 2048], P(None, 'row', 'col')
- pend_y: float32 [2, 4, 64, 2048], P(None, 'row', None, 'col')
- pend_z: float32 [2, 4, 64, 2048], P(None, 'row', None, 'col')
The draws below stay inside these ranges and needn't reach their ends.
Inputs may be any that keep to these rules, and one draw needn't show every extreme that they name: `ranks`: ranks_ij leading columns of tile (i, j)'s left factor are in use.
All inputs are finite; a program needn't handle non-finite values.
Results may differ from the reference program's by a relative error of at most 0.0003.
Values sent between devices are 32-bit elements; how exact they have to be, the bound alone decides.
A program may use at most 64 MiB of HBM per device.

```python
import math
import jax
import jax.numpy as jnp
from jax import lax

NB = 2048
K = 64
M = 8
TPR = 2
N_ROW = 4
N_COL = 8


def plant(result, own_key, least, top_value):
    spot = [jax.random.randint(jax.random.fold_in(own_key, axis), (), 0, length) for axis, length in enumerate(result.shape)]
    widest = result.shape.index(max(result.shape))
    beside = spot[:widest] + [(spot[widest] + 1) % result.shape[widest]] + spot[widest + 1:]
    return result.at[tuple(spot)].set(least).at[tuple(beside)].set(top_value)


def level_of(key, extent, pieces, least, top_value):
    factor_of = 1.0
    for dim, shards_of in pieces:
        heights = jax.random.uniform(jax.random.fold_in(jax.random.fold_in(key, 6), dim), (shards_of,), jnp.float32, least / len(pieces), top_value / len(pieces))
        factor_of = factor_of * jnp.repeat(jnp.exp(heights), extent[dim] // shards_of).reshape((-1,) + (1,) * (len(extent) - 1 - dim))
    return factor_of


def scatter_about(own_key, shape, width, most, split=(), kind=jnp.bfloat16):
    loudness = level_of(own_key, shape, split, -0.22, 0.18) if split else 1.0
    values = jax.random.normal(own_key, shape, jnp.float32) * width * loudness
    return jnp.minimum(jnp.maximum(values, -most), most).astype(kind)


def setup_inputs(seed: int = 0) -> dict:
    key_of = jax.random.split(jax.random.key(seed), 9)
    trail_u = scatter_about(key_of[0], (TPR, N_ROW, N_COL, K, NB), 1.0, 6.0, ((1, 4), (2, 8)), jnp.float32)
    trail_v = scatter_about(key_of[1], (TPR, N_ROW, N_COL, K, NB), K ** -0.5, 0.75, ((1, 4), (2, 8)), jnp.float32)
    ranks = plant(jax.random.randint(key_of[2], (TPR, N_ROW, N_COL), K // 4, K + 1), jax.random.fold_in(key_of[2], 1), K // 4, K).astype(jnp.int32)
    panel_u = scatter_about(key_of[3], (TPR, N_ROW, K, NB), 1.0, 6.0, ((1, 4), (3, 8)), jnp.float32)
    panel_v = scatter_about(key_of[4], (TPR, N_ROW, K, NB), NB ** -0.5, 0.125, ((1, 4), (3, 8)), jnp.float32)
    locations = jnp.clip(1.0 * jax.random.uniform(key_of[5], (TPR, N_ROW, 2, NB), jnp.float32) ** level_of(key_of[5], (TPR, N_ROW, 2, NB), ((1, 4), (3, 8)), -0.2, 0.2), 0.0, 1.0)
    pend_locs = jnp.clip(1.0 * jax.random.uniform(key_of[6], (2, NB), jnp.float32) ** level_of(key_of[6], (2, NB), ((1, 8),), -0.2, 0.2), 0.0, 1.0)
    sketch = scatter_about(key_of[7], (K, NB), NB ** -0.5, 0.125, (), jnp.float32)
    return {"trail_u": trail_u, "trail_v": trail_v, "ranks": ranks, "panel_u": panel_u, "panel_v": panel_v, "locations": locations, "pend_locs": pend_locs, "sketch": sketch}


matern_scale = 4.0
length_scale = 0.15
root_three = math.sqrt(3.0)

def matmul(left, right):
    return jnp.dot(left, right, precision=lax.Precision.HIGHEST, preferred_element_type=jnp.float32)

def matern(row_points, col_points):
    delta_x = row_points[0][:, None] - col_points[0][None, :]
    delta_y = row_points[1][:, None] - col_points[1][None, :]
    distance = jnp.sqrt(delta_x * delta_x + delta_y * delta_y)
    scaled = root_three * distance / length_scale
    return matern_scale * (1.0 + scaled) * jnp.exp(-scaled)

def reference(trail_u, trail_v, ranks, panel_u, panel_v, locations, pend_locs, sketch):
    whole_u = panel_u.reshape(M, K, NB)
    whole_v = panel_v.reshape(M, K, NB)
    flat_u = trail_u.reshape(M * N_COL, K, NB)
    flat_v = trail_v.reshape(M * N_COL, K, NB)
    flat_rank = ranks.reshape(M * N_COL)

    def one_tile(flat_index):
        row_tile = flat_index // N_COL
        col_tile = flat_index % N_COL
        in_use = (jnp.arange(K, dtype=jnp.int32) < flat_rank[flat_index]).astype(jnp.float32)
        u_tile = flat_u[flat_index] * in_use[:, None]
        v_tile = flat_v[flat_index]
        row_pu = whole_u[row_tile]
        row_pv = whole_v[row_tile]
        col_pu = whole_u[col_tile]
        col_pv = whole_v[col_tile]
        v_sketch = matmul(v_tile, sketch.T)
        u_sketch = matmul(u_tile, sketch.T)
        cross_gram = matmul(row_pv, col_pv.T)
        col_sketch = matmul(col_pu, sketch.T)
        row_sketch = matmul(row_pu, sketch.T)
        y_tile = matmul(v_sketch.T, u_tile) - matmul(matmul(cross_gram, col_sketch).T, row_pu)
        z_tile = matmul(u_sketch.T, v_tile) - matmul(matmul(row_sketch.T, cross_gram), col_pu)
        keep_tile = row_tile > col_tile
        return (jnp.where(keep_tile, y_tile, 0.0), jnp.where(keep_tile, z_tile, 0.0))
    trail_y, trail_z = lax.map(one_tile, jnp.arange(M * N_COL, dtype=jnp.int32))

    def one_pending(row_points):
        kernel = matern(row_points, pend_locs)
        return (matmul(sketch, kernel.T), matmul(sketch, kernel))
    pend_y, pend_z = lax.map(one_pending, locations.reshape(M, 2, NB))
    return (trail_y.reshape(TPR, N_ROW, N_COL, K, NB), trail_z.reshape(TPR, N_ROW, N_COL, K, NB), pend_y.reshape(TPR, N_ROW, K, NB), pend_z.reshape(TPR, N_ROW, K, NB))
```

```python
import functools
import math

import jax
import jax.numpy as jnp
from jax import lax
from jax.experimental import pallas as pl
from jax.experimental.pallas import tpu as pltpu
from jax.sharding import PartitionSpec as P

matern_scale = 4.0
length_scale = 0.15
root_three = math.sqrt(3.0)
point_scale = root_three / length_scale
log2_e = math.log2(math.e)
smallest = 1e-30

MESH = pl.DeviceIdType.MESH
NN = (((1,), (0,)), ((), ()))
NT = (((1,), (1,)), ((), ()))
SLAB = 16


def halves(value):
    high = value.astype(jnp.bfloat16)
    low = (value - high.astype(jnp.float32)).astype(jnp.bfloat16)
    return high, low


def product(left, right, dims):
    return lax.dot_general(left, right, dims, preferred_element_type=jnp.float32)


def dot3_split(left_both, right, dims):
    rows = left_both.shape[0] // 2
    right_high, right_low = halves(right)
    both = product(left_both, right_high, dims)
    return both[:rows] + both[rows:] + product(left_both[:rows], right_low, dims)


def dot3(left, right, dims):
    left_high, left_low = halves(left)
    return dot3_split(jnp.concatenate([left_high, left_low], axis=0), right, dims)


def kernel(
    n_row, n_col,
    ranks, trail_u, trail_v, panel_u, panel_v, locs, pend, sketch,
    trail_y, trail_z, pend_y, pend_z,
    u_buf, v_buf, loc_all, pend_all, pu_all, pj_all, pv_all, g_part, g_all,
    points, own_points, sk_both, mat_high, mat_low, acc, vs_acc, us_acc, rs_acc, cs_acc,
    local_sem, loc_send, loc_recv, pend_send, pend_recv, pu_send, pu_recv,
    pj_send, pj_recv, pv_send, pv_recv, g_send, g_recv,
):
    row, col = lax.axis_index("row"), lax.axis_index("col")
    n_z = n_col // 2
    z_pos, core = col // 2, col % 2
    owner_row, owner_slot = col % n_row, col // n_row
    is_owner = row == owner_row
    slots, rank_dim, width = u_buf.shape
    w = panel_u.shape[2]
    flat = slots * rank_dim

    copy_u = pltpu.make_async_copy(trail_u, u_buf, local_sem.at[0])
    copy_v = pltpu.make_async_copy(trail_v, v_buf, local_sem.at[1])
    copy_u.start()
    copy_v.start()

    barrier = pltpu.get_barrier_semaphore()
    for step in range(1, n_col):
        pl.semaphore_signal(
            barrier, inc=1, device_id=(row, (col + step) % n_col), device_id_type=MESH)
    for step in range(1, n_row):
        pl.semaphore_signal(
            barrier, inc=1, device_id=((row + step) % n_row, col), device_id_type=MESH)

    def remote(src, dst, send, recv, to_row, to_col):
        return pltpu.make_async_remote_copy(
            src_ref=src, dst_ref=dst, send_sem=send, recv_sem=recv,
            device_id=(to_row, to_col), device_id_type=MESH)

    def loc_copy(source, step):
        return remote(locs, loc_all.at[source], loc_send.at[step], loc_recv.at[source],
                      row, (col + step) % n_col)

    def pend_copy(source, step):
        return remote(pend, pend_all.at[source], pend_send.at[step], pend_recv.at[source],
                      row, (col + step) % n_col)

    def pv_copy(source, step):
        return remote(panel_v, pv_all.at[source], pv_send.at[step], pv_recv.at[source],
                      (row + step) % n_row, col)

    def pu_copy(block, way, own=False):
        to_col = (col - 2, col + 2, 2 * z_pos + 1 - core)[way]
        src = panel_u if own else pu_all.at[block]
        return remote(src, pu_all.at[block], pu_send.at[way, block], pu_recv.at[block],
                      row, to_col)

    def pj_copy(block, step, own=False):
        src = panel_u.at[owner_slot] if own else pu_all.at[block, owner_slot]
        return remote(src, pj_all.at[block], pj_send.at[step, block], pj_recv.at[block],
                      (row + step) % n_row, col)

    def g_copy(source, step):
        target = (col + step) % n_col
        return remote(g_part.at[target], g_all.at[source], g_send.at[step], g_recv.at[source],
                      row, target)

    def to_rows(block, own=False):
        @pl.when(is_owner)
        def _():
            for step in range(1, n_row):
                pj_copy(block, step, own).start()

    sk_all = sketch[...]
    sk_high, sk_low = halves(sk_all)
    for block in range(n_col):
        sk_both[block, 0:rank_dim] = sk_high[:, block * w:(block + 1) * w]
        sk_both[block, rank_dim:2 * rank_dim] = sk_low[:, block * w:(block + 1) * w]

    pl.semaphore_wait(barrier, n_col - 1 + n_row - 1)

    for step in range(1, n_col):
        loc_copy(col, step).start()
        pend_copy(col, step).start()

    @pl.when(z_pos > 0)
    def _():
        pu_copy(col, 0, True).start()

    @pl.when(z_pos < n_z - 1)
    def _():
        pu_copy(col, 1, True).start()

    for step in range(1, n_row):
        pv_copy(row, step).start()
    pu_copy(col, 2, True).start()
    to_rows(col, True)

    pu_all[col] = panel_u[...]
    pv_all[row] = panel_v[...]
    loc_all[col] = locs[...]
    pend_all[col] = pend[...]
    acc[...] = jnp.zeros_like(acc)
    vs_acc[...] = jnp.zeros_like(vs_acc)
    us_acc[...] = jnp.zeros_like(us_acc)
    rs_acc[...] = jnp.zeros_like(rs_acc)
    cs_acc[...] = jnp.zeros_like(cs_acc)

    copy_u.wait()
    copy_v.wait()
    rank_iota = lax.broadcasted_iota(jnp.int32, (rank_dim, 1), 0)
    for slot in range(slots):
        in_use = rank_iota < ranks[slot, 0, 0]
        u_buf[slot] = jnp.where(in_use, u_buf[slot], 0.0)

    @pl.loop(0, n_col)
    def _(block):
        lanes = pl.ds(pl.multiple_of(block * w, w), w)
        sk = sk_both[block]
        vs_acc[...] += dot3_split(sk, v_buf[:, :, lanes].reshape(flat, w), NT)
        us_acc[...] += dot3_split(sk, u_buf[:, :, lanes].reshape(flat, w), NT)

    own_points[0:1, :] = jnp.concatenate(
        [locs[slot, 0:1] for slot in range(slots)] + [pend[0:1]] * slots, axis=1) * point_scale
    own_points[1:2, :] = jnp.concatenate(
        [locs[slot, 1:2] for slot in range(slots)] + [pend[1:2]] * slots, axis=1) * point_scale
    pad_rows = points.shape[2] - 2 * slots - 2

    def chunk(step):
        block = lax.rem(col + step, n_col)

        @pl.when(step > 0)
        def _():
            loc_copy(block, 1).wait_recv()
            pend_copy(block, 1).wait_recv()

        stack = [loc_all[block, slot] for slot in range(slots)] + [pend_all[block]]
        if pad_rows:
            stack.append(jnp.zeros((pad_rows, w), jnp.float32))
        points[0] = jnp.concatenate(stack, axis=0).T * point_scale

        @pl.loop(0, w // SLAB)
        def _(slab):
            rows = pl.ds(pl.multiple_of(slab * SLAB, SLAB), SLAB)
            at = points[0, rows, :]
            for part in range(2 * slots):
                base = 2 * slots if part < slots else 2 * (part - slots)
                lanes = slice(part * w, (part + 1) * w)
                delta_x = at[:, base:base + 1] - own_points[0:1, lanes]
                delta_y = at[:, base + 1:base + 2] - own_points[1:2, lanes]
                square = delta_x * delta_x + delta_y * delta_y
                scaled = square * lax.rsqrt(jnp.maximum(square, smallest))
                value = (1.0 + scaled) * jnp.exp2(scaled * -log2_e)
                high, low = halves(value)
                mat_high[rows, lanes] = high
                mat_low[rows, lanes] = low

        sk = sk_both[block]
        both = product(sk, mat_high[...], NN)
        acc[...] += (both[:rank_dim] + both[rank_dim:]
                     + product(sk[:rank_dim], mat_low[...], NN))

    def chunks(first, last):
        pl.loop(first, last)(chunk)

    def relay(distance):
        @pl.when(z_pos + distance < n_z)
        def _():
            block = col + 2 * distance
            pu_copy(block, 2).wait_recv()

            @pl.when(z_pos > 0)
            def _():
                pu_copy(block, 0).start()
            pu_copy(block, 2).start()
            to_rows(block)

        @pl.when(z_pos - distance >= 0)
        def _():
            block = col - 2 * distance
            pu_copy(block, 2).wait_recv()

            @pl.when(z_pos < n_z - 1)
            def _():
                pu_copy(block, 1).start()
            pu_copy(block, 2).start()
            to_rows(block)

    def from_partner(distance):
        other = 2 * z_pos + 1 - core

        @pl.when(z_pos + distance < n_z)
        def _():
            block = other + 2 * distance
            pu_copy(block, 2).wait_recv()
            to_rows(block)

        if distance:
            @pl.when(z_pos - distance >= 0)
            def _():
                block = other - 2 * distance
                pu_copy(block, 2).wait_recv()
                to_rows(block)

    def cut(piece, pieces):
        return piece * n_col // pieces

    chunks(0, cut(1, 8))
    from_partner(0)
    chunks(cut(1, 8), cut(2, 8))
    relay(1)
    for step in range(1, n_row):
        pv_copy((row + step) % n_row, 1).wait_recv()
    own_v = panel_v[...].reshape(flat, w)
    for source in range(n_row):
        for slot in range(slots):
            tile = slot * n_row + source
            if tile < n_col:
                g_part[tile] = dot3(pv_all[source, slot], own_v, NT)
    chunks(cut(2, 8), cut(3, 8))
    for step in range(1, n_col):
        g_copy(col, step).start()
    g_all[col] = g_part[col]
    from_partner(1)
    chunks(cut(3, 8), cut(4, 8))
    for distance in range(2, n_z):
        relay(distance)
        if distance > 2:
            from_partner(distance - 1)
        if distance == 2:
            chunks(cut(4, 8), cut(6, 8))
    chunks(cut(6, 8), n_col)
    if n_z > 1:
        from_partner(n_z - 1)

    @pl.when(is_owner)
    def _():
        @pl.loop(0, n_col)
        def _(block):
            pj_all[block] = pu_all[block, owner_slot]

    for slot in range(slots):
        pend_y[slot, 0] = acc[:, slot * w:(slot + 1) * w] * matern_scale
        pend_z[slot, 0] = acc[:, (slots + slot) * w:(slots + slot + 1) * w] * matern_scale

    @pl.loop(0, n_col)
    def _(block):
        rs_acc[...] += dot3_split(sk_both[block], pu_all[block].reshape(flat, w), NT)

    for step in range(1, n_col):
        g_copy((col + step) % n_col, 1).wait_recv()
    gram = g_all[0]
    for block in range(1, n_col):
        gram = gram + g_all[block]

    @pl.when(jnp.logical_not(is_owner))
    def _():
        @pl.loop(0, n_col)
        def _(block):
            pj_copy(block, 1).wait_recv()

    @pl.loop(0, n_col)
    def _(block):
        cs_acc[...] += dot3_split(sk_both[block], pj_all[block], NT)

    left_core = dot3(cs_acc[...], gram, NN)
    for slot in range(slots):
        lanes = slice(slot * rank_dim, (slot + 1) * rank_dim)
        right_core = dot3(rs_acc[:, lanes], gram[:, lanes], NT)
        y_high, y_low = halves(jnp.concatenate([vs_acc[:, lanes], -left_core[:, lanes]], axis=1))
        z_high, z_low = halves(jnp.concatenate([us_acc[:, lanes], -right_core], axis=1))
        y_both = jnp.concatenate([y_high, y_low], axis=0)
        z_both = jnp.concatenate([z_high, z_low], axis=0)
        active = slot * n_row + row > col

        @pl.when(active)
        def _(slot=slot, y_both=y_both, z_both=z_both):
            @pl.loop(0, n_col)
            def _(block):
                cols = pl.ds(pl.multiple_of(block * w, w), w)
                y_right = jnp.concatenate([u_buf[slot, :, cols], pu_all[block, slot]], axis=0)
                trail_y[slot, 0, 0, :, cols] = dot3_split(y_both, y_right, NN)
                z_right = jnp.concatenate([v_buf[slot, :, cols], pj_all[block]], axis=0)
                trail_z[slot, 0, 0, :, cols] = dot3_split(z_both, z_right, NN)

        @pl.when(jnp.logical_not(active))
        def _(slot=slot):
            trail_y[slot, 0, 0] = jnp.zeros((rank_dim, width), jnp.float32)
            trail_z[slot, 0, 0] = jnp.zeros((rank_dim, width), jnp.float32)

    for step in range(1, n_col):
        loc_copy(col, step).wait_send()
        pend_copy(col, step).wait_send()
        g_copy(col, step).wait_send()
    for step in range(1, n_row):
        pv_copy(row, step).wait_send()
    for distance in range(n_z):
        @pl.when(z_pos + distance < n_z)
        def _(distance=distance):
            block = col + 2 * distance
            pu_copy(block, 2).wait_send()

            @pl.when(z_pos > 0)
            def _():
                pu_copy(block, 0).wait_send()

        @pl.when(z_pos - distance >= 0)
        def _(distance=distance):
            block = col - 2 * distance
            if distance:
                pu_copy(block, 2).wait_send()

            @pl.when(z_pos < n_z - 1)
            def _():
                pu_copy(block, 1).wait_send()

    @pl.when(is_owner)
    def _():
        @pl.loop(0, n_col)
        def _(block):
            for step in range(1, n_row):
                pj_copy(block, step).wait_send()


def broadcast(block, axis, owner):
    block = jnp.where(lax.axis_index(axis) == owner, block, jnp.zeros_like(block))
    return lax.psum(block, axis)


def matmul(left, right):
    return jnp.dot(left, right, precision=lax.Precision.HIGHEST, preferred_element_type=jnp.float32)


def batched(form, left, right):
    return jnp.einsum(
        form, left, right, precision=lax.Precision.HIGHEST, preferred_element_type=jnp.float32
    )


def matern(row_points, col_points):
    delta_x = row_points[0][:, None] - col_points[0][None, :]
    delta_y = row_points[1][:, None] - col_points[1][None, :]
    distance = jnp.sqrt(delta_x * delta_x + delta_y * delta_y)
    scaled = root_three * distance / length_scale
    return matern_scale * (1.0 + scaled) * jnp.exp(-scaled)


def plain_on_device(trail_u, trail_v, ranks, panel_u, panel_v, locations, pend_locs, sketch):
    row_count = lax.axis_size("row")
    row_index = lax.axis_index("row")
    col_index = lax.axis_index("col")
    row_slots = trail_u.shape[0]
    rank_dim = trail_u.shape[3]
    width = trail_u.shape[4]
    local_width = pend_locs.shape[1]
    gathered_u, gathered_v = (
        lax.all_gather(panel_u, "col", axis=3, tiled=True),
        lax.all_gather(panel_v, "col", axis=3, tiled=True),
    )
    slot_index = col_index // row_count
    own_u = lax.dynamic_index_in_dim(gathered_u[:, 0], slot_index, 0, keepdims=False)
    own_v = lax.dynamic_index_in_dim(gathered_v[:, 0], slot_index, 0, keepdims=False)
    col_pu, col_pv = (
        broadcast(own_u, "row", col_index % row_count),
        broadcast(own_v, "row", col_index % row_count),
    )
    rank_iota = lax.broadcasted_iota(jnp.int32, (row_slots, rank_dim), 1)
    in_use = (rank_iota < ranks[:, 0, 0][:, None]).astype(jnp.float32)
    u_tiles = trail_u[:, 0, 0] * in_use[:, :, None]
    v_tiles = trail_v[:, 0, 0]
    row_pu = gathered_u[:, 0]
    row_pv = gathered_v[:, 0]
    v_sketch = batched("tkn,ln->tkl", v_tiles, sketch)
    u_sketch = batched("tkn,ln->tkl", u_tiles, sketch)
    cross_gram = batched("tkn,ln->tkl", row_pv, col_pv)
    col_sketch = matmul(col_pu, sketch.T)
    row_sketch = batched("tkn,ln->tkl", row_pu, sketch)
    left_core = batched("tkm,ml->tkl", cross_gram, col_sketch)
    y_tiles = batched("tkl,tkn->tln", v_sketch, u_tiles) - batched(
        "tkl,tkn->tln", left_core, row_pu
    )
    right_core = batched("tkl,tkm->tlm", row_sketch, cross_gram)
    z_tiles = batched("tkl,tkn->tln", u_sketch, v_tiles) - batched(
        "tlm,mn->tln", right_core, col_pu
    )
    tile_rows = jnp.arange(row_slots, dtype=jnp.int32) * row_count + row_index
    keep_mask = (tile_rows > col_index)[:, None, None]
    trail_y = jnp.where(keep_mask, y_tiles, 0.0).reshape(row_slots, 1, 1, rank_dim, width)
    trail_z = jnp.where(keep_mask, z_tiles, 0.0).reshape(row_slots, 1, 1, rank_dim, width)
    y_list = []
    z_list = []
    rows_all, pend_all = (
        lax.all_gather(locations, "col", axis=3, tiled=True),
        lax.all_gather(pend_locs.reshape(1, 1, 2, local_width), "col", axis=3, tiled=True),
    )
    col_points = pend_all[0, 0]
    for slot_num in range(row_slots):
        own_kernel = matern(locations[slot_num, 0], col_points)
        y_list.append(matmul(sketch, own_kernel.T))
        col_kernel = matern(rows_all[slot_num, 0], pend_locs)
        z_list.append(matmul(sketch, col_kernel))
    pend_y = jnp.stack(y_list)
    pend_z = jnp.stack(z_list)
    pend_y = pend_y.reshape(row_slots, 1, rank_dim, local_width)
    pend_z = pend_z.reshape(row_slots, 1, rank_dim, local_width)
    return (trail_y, trail_z, pend_y, pend_z)


def on_device(n_row, n_col, trail_u, trail_v, ranks, panel_u, panel_v, locations, pend_locs, sketch):
    slots, _, _, rank_dim, width = trail_u.shape
    w = pend_locs.shape[1]
    if w % 128 or rank_dim % 16 or n_col % 2:
        return plain_on_device(
            trail_u, trail_v, ranks, panel_u, panel_v, locations, pend_locs, sketch
        )
    flat = slots * rank_dim
    f32, bf16 = jnp.float32, jnp.bfloat16
    dma = pltpu.SemaphoreType.DMA
    vmem = pl.BlockSpec(memory_space=pltpu.VMEM)
    hbm = pl.BlockSpec(memory_space=pl.ANY)
    point_rows = -(-(2 * slots + 2) // 8) * 8
    return pl.pallas_call(
        functools.partial(kernel, n_row, n_col),
        out_shape=(
            jax.ShapeDtypeStruct(trail_u.shape, f32),
            jax.ShapeDtypeStruct(trail_v.shape, f32),
            jax.ShapeDtypeStruct(panel_u.shape, f32),
            jax.ShapeDtypeStruct(panel_u.shape, f32),
        ),
        in_specs=[pl.BlockSpec(memory_space=pltpu.SMEM), hbm, hbm] + [vmem] * 5,
        out_specs=(vmem,) * 4,
        scratch_shapes=[
            pltpu.VMEM((slots, rank_dim, width), f32),
            pltpu.VMEM((slots, rank_dim, width), f32),
            pltpu.VMEM((n_col, slots, 2, w), f32),
            pltpu.VMEM((n_col, 2, w), f32),
            pltpu.VMEM((n_col, slots, rank_dim, w), f32),
            pltpu.VMEM((n_col, rank_dim, w), f32),
            pltpu.VMEM((n_row, slots, rank_dim, w), f32),
            pltpu.VMEM((n_col, rank_dim, flat), f32),
            pltpu.VMEM((n_col, rank_dim, flat), f32),
            pltpu.VMEM((1, w, point_rows), f32),
            pltpu.VMEM((2, 2 * slots * w), f32),
            pltpu.VMEM((n_col, 2 * rank_dim, w), bf16),
            pltpu.VMEM((w, 2 * slots * w), bf16),
            pltpu.VMEM((w, 2 * slots * w), bf16),
            pltpu.VMEM((rank_dim, 2 * slots * w), f32),
            pltpu.VMEM((rank_dim, flat), f32),
            pltpu.VMEM((rank_dim, flat), f32),
            pltpu.VMEM((rank_dim, flat), f32),
            pltpu.VMEM((rank_dim, rank_dim), f32),
            dma((2,)),
            dma((n_col,)), dma((n_col,)), dma((n_col,)), dma((n_col,)),
            dma((3, n_col)), dma((n_col,)),
            dma((n_row, n_col)), dma((n_col,)),
            dma((n_row,)), dma((n_row,)),
            dma((n_col,)), dma((n_col,)),
        ],
        compiler_params=pltpu.CompilerParams(collective_id=0, has_side_effects=True),
    )(
        ranks,
        trail_u.reshape(slots, rank_dim, width),
        trail_v.reshape(slots, rank_dim, width),
        panel_u.reshape(slots, rank_dim, w),
        panel_v.reshape(slots, rank_dim, w),
        locations.reshape(slots, 2, w),
        pend_locs,
        sketch,
    )


def solution(mesh):
    in_specs = (
        P(None, "row", "col", None, None),
        P(None, "row", "col", None, None),
        P(None, "row", "col"),
        P(None, "row", None, "col"),
        P(None, "row", None, "col"),
        P(None, "row", None, "col"),
        P(None, "col"),
        P(),
    )
    out_specs = (
        P(None, "row", "col", None, None),
        P(None, "row", "col", None, None),
        P(None, "row", None, "col"),
        P(None, "row", None, "col"),
    )
    body = functools.partial(on_device, mesh.shape["row"], mesh.shape["col"])
    return jax.shard_map(
        body, mesh=mesh, in_specs=in_specs, out_specs=out_specs, check_vma=False
    )
```

```python
import functools
import math

import jax
import jax.numpy as jnp
from jax import lax
from jax.experimental import pallas as pl
from jax.experimental.pallas import tpu as pltpu
from jax.sharding import PartitionSpec as P

matern_scale = 4.0
length_scale = 0.15
root_three = math.sqrt(3.0)
point_scale = root_three / length_scale
log2_e = math.log2(math.e)
smallest = 1e-30

MESH = pl.DeviceIdType.MESH
NN = (((1,), (0,)), ((), ()))
NT = (((1,), (1,)), ((), ()))
SLAB = 16
UNROLL = 8


def halves(value):
    high = value.astype(jnp.bfloat16)
    low = (value - high.astype(jnp.float32)).astype(jnp.bfloat16)
    return high, low


def product(left, right, dims):
    return lax.dot_general(left, right, dims, preferred_element_type=jnp.float32)


def dot3_split(left_both, right, dims):
    rows = left_both.shape[0] // 2
    right_high, right_low = halves(right)
    both = product(left_both, right_high, dims)
    return both[:rows] + both[rows:] + product(left_both[:rows], right_low, dims)


def dot3(left, right, dims):
    left_high, left_low = halves(left)
    return dot3_split(jnp.concatenate([left_high, left_low], axis=0), right, dims)


def kernel(
    n_row, n_col,
    ranks, trail_u, trail_v, panel_u, panel_v, locs, pend, sketch,
    pu_out, pj_out, acc, y_left, z_left,
    u_buf, v_buf, loc_all, pend_all, pu_all, pj_all, pv_all, g_part, g_all,
    points, own_points, sk_both, mat_high, mat_low, own_sketches,
    local_sem, loc_send, loc_recv, pend_send, pend_recv, pu_send, pu_recv,
    pj_send, pj_recv, pv_send, pv_recv, g_send, g_recv,
):
    row, col = lax.axis_index("row"), lax.axis_index("col")
    n_z = n_col // 2
    z_pos, core = col // 2, col % 2
    owner_row, owner_slot = col % n_row, col // n_row
    is_owner = row == owner_row
    slots, rank_dim, width = u_buf.shape
    w = panel_u.shape[2]
    flat = slots * rank_dim

    copy_u = pltpu.make_async_copy(trail_u, u_buf, local_sem.at[0])
    copy_v = pltpu.make_async_copy(trail_v, v_buf, local_sem.at[1])
    copy_u.start()
    copy_v.start()

    barrier = pltpu.get_barrier_semaphore()
    for step in range(1, n_col):
        pl.semaphore_signal(
            barrier, inc=1, device_id=(row, (col + step) % n_col), device_id_type=MESH)
    for step in range(1, n_row):
        pl.semaphore_signal(
            barrier, inc=1, device_id=((row + step) % n_row, col), device_id_type=MESH)

    def remote(src, dst, send, recv, to_row, to_col):
        return pltpu.make_async_remote_copy(
            src_ref=src, dst_ref=dst, send_sem=send, recv_sem=recv,
            device_id=(to_row, to_col), device_id_type=MESH)

    def loc_copy(source, step):
        return remote(locs, loc_all.at[source], loc_send.at[step], loc_recv.at[source],
                      row, (col + step) % n_col)

    def pend_copy(source, step):
        return remote(pend, pend_all.at[source], pend_send.at[step], pend_recv.at[source],
                      row, (col + step) % n_col)

    def pv_copy(source, step):
        return remote(panel_v, pv_all.at[source], pv_send.at[step], pv_recv.at[source],
                      (row + step) % n_row, col)

    def pu_copy(block, way, own=False):
        to_col = (col - 2, col + 2, 2 * z_pos + 1 - core)[way]
        src = panel_u if own else pu_all.at[block]
        return remote(src, pu_all.at[block], pu_send.at[way, block], pu_recv.at[block],
                      row, to_col)

    def pj_copy(block, step, own=False):
        src = panel_u.at[owner_slot] if own else pu_all.at[block, owner_slot]
        return remote(src, pj_all.at[block], pj_send.at[step, block], pj_recv.at[block],
                      (row + step) % n_row, col)

    def g_copy(source, step):
        target = (col + step) % n_col
        return remote(g_part.at[target], g_all.at[source], g_send.at[step], g_recv.at[source],
                      row, target)

    def to_rows(block, own=False):
        @pl.when(is_owner)
        def _():
            for step in range(1, n_row):
                pj_copy(block, step, own).start()

    sk_all = sketch[...]
    sk_high, sk_low = halves(sk_all)
    for block in range(n_col):
        sk_both[block, 0:rank_dim] = sk_high[:, block * w:(block + 1) * w]
        sk_both[block, rank_dim:2 * rank_dim] = sk_low[:, block * w:(block + 1) * w]

    pl.semaphore_wait(barrier, n_col - 1 + n_row - 1)

    for step in range(1, n_col):
        loc_copy(col, step).start()
        pend_copy(col, step).start()

    @pl.when(z_pos > 0)
    def _():
        pu_copy(col, 0, True).start()

    @pl.when(z_pos < n_z - 1)
    def _():
        pu_copy(col, 1, True).start()

    for step in range(1, n_row):
        pv_copy(row, step).start()
    pu_copy(col, 2, True).start()
    to_rows(col, True)

    pu_all[col] = panel_u[...]
    pv_all[row] = panel_v[...]
    loc_all[col] = locs[...]
    pend_all[col] = pend[...]
    acc[...] = jnp.zeros_like(acc)

    copy_u.wait()
    copy_v.wait()
    rank_iota = lax.broadcasted_iota(jnp.int32, (rank_dim, 1), 0)
    in_use = [rank_iota < ranks[slot] for slot in range(slots)]
    v_sketch = jnp.zeros((rank_dim, flat), jnp.float32)
    u_sketch = jnp.zeros((rank_dim, flat), jnp.float32)
    for block in range(n_col):
        lanes = slice(block * w, (block + 1) * w)
        sk = sk_both[block]
        v_sketch += dot3_split(sk, v_buf[:, :, lanes].reshape(flat, w), NT)
        u_block = [jnp.where(in_use[slot], u_buf[slot, :, lanes], 0.0) for slot in range(slots)]
        u_sketch += dot3_split(sk, jnp.concatenate(u_block, axis=0), NT)
    own_sketches[0] = v_sketch
    own_sketches[1] = u_sketch

    own_points[0:1, :] = jnp.concatenate(
        [locs[slot, 0:1] for slot in range(slots)] + [pend[0:1]] * slots, axis=1) * point_scale
    own_points[1:2, :] = jnp.concatenate(
        [locs[slot, 1:2] for slot in range(slots)] + [pend[1:2]] * slots, axis=1) * point_scale
    pad_rows = points.shape[2] - 2 * slots - 2

    def chunk(step):
        block = lax.rem(col + step, n_col)

        @pl.when(step > 0)
        def _():
            loc_copy(block, 1).wait_recv()
            pend_copy(block, 1).wait_recv()

        stack = [loc_all[block, slot] for slot in range(slots)] + [pend_all[block]]
        if pad_rows:
            stack.append(jnp.zeros((pad_rows, w), jnp.float32))
        points[0] = jnp.concatenate(stack, axis=0).T * point_scale

        @pl.loop(0, w // SLAB, unroll=UNROLL)
        def _(slab):
            rows = pl.ds(pl.multiple_of(slab * SLAB, SLAB), SLAB)
            at = points[0, rows, :]
            for part in range(2 * slots):
                base = 2 * slots if part < slots else 2 * (part - slots)
                lanes = slice(part * w, (part + 1) * w)
                delta_x = at[:, base:base + 1] - own_points[0:1, lanes]
                delta_y = at[:, base + 1:base + 2] - own_points[1:2, lanes]
                square = delta_x * delta_x + delta_y * delta_y
                scaled = square * lax.rsqrt(jnp.maximum(square, smallest))
                value = (1.0 + scaled) * jnp.exp2(scaled * -log2_e)
                high, low = halves(value)
                mat_high[rows, lanes] = high
                mat_low[rows, lanes] = low

        sk = sk_both[block]
        both = product(sk, mat_high[...], NN)
        acc[...] += (both[:rank_dim] + both[rank_dim:]
                     + product(sk[:rank_dim], mat_low[...], NN))

    def chunks(first, last):
        pl.loop(first, last)(chunk)

    def relay(distance):
        @pl.when(z_pos + distance < n_z)
        def _():
            block = col + 2 * distance
            pu_copy(block, 2).wait_recv()

            @pl.when(z_pos > 0)
            def _():
                pu_copy(block, 0).start()
            pu_copy(block, 2).start()
            to_rows(block)

        @pl.when(z_pos - distance >= 0)
        def _():
            block = col - 2 * distance
            pu_copy(block, 2).wait_recv()

            @pl.when(z_pos < n_z - 1)
            def _():
                pu_copy(block, 1).start()
            pu_copy(block, 2).start()
            to_rows(block)

    def from_partner(distance):
        other = 2 * z_pos + 1 - core

        @pl.when(z_pos + distance < n_z)
        def _():
            block = other + 2 * distance
            pu_copy(block, 2).wait_recv()
            to_rows(block)

        if distance:
            @pl.when(z_pos - distance >= 0)
            def _():
                block = other - 2 * distance
                pu_copy(block, 2).wait_recv()
                to_rows(block)

    def cut(piece, pieces):
        return piece * n_col // pieces

    from_partner(0)
    chunks(0, cut(1, 8))
    relay(1)
    chunks(cut(1, 8), cut(2, 8))
    for step in range(1, n_row):
        pv_copy((row + step) % n_row, 1).wait_recv()
    own_v = panel_v[...].reshape(flat, w)
    for source in range(n_row):
        for slot in range(slots):
            tile = slot * n_row + source
            if tile < n_col:
                g_part[tile] = dot3(pv_all[source, slot], own_v, NT)
    from_partner(1)
    chunks(cut(2, 8), cut(3, 8))
    for step in range(1, n_col):
        g_copy(col, step).start()
    g_all[col] = g_part[col]
    done = cut(3, 8)
    for distance in range(2, n_z):
        relay(distance)
        if distance > 2:
            from_partner(distance - 1)
        upto = min(done + cut(2, 8), n_col)
        chunks(done, upto)
        done = upto
    if n_z > 2:
        from_partner(n_z - 1)
    chunks(done, n_col)

    @pl.when(is_owner)
    def _():
        @pl.loop(0, n_col)
        def _(block):
            pj_all[block] = pu_all[block, owner_slot]

    pu_store = pltpu.make_async_copy(pu_all, pu_out, local_sem.at[0])
    pu_store.start()
    row_sketch = jnp.zeros((rank_dim, flat), jnp.float32)
    for block in range(n_col):
        row_sketch += dot3_split(sk_both[block], pu_all[block].reshape(flat, w), NT)

    for step in range(1, n_col):
        g_copy((col + step) % n_col, 1).wait_recv()
    gram = g_all[0]
    for block in range(1, n_col):
        gram = gram + g_all[block]

    @pl.when(jnp.logical_not(is_owner))
    def _():
        @pl.loop(0, n_col)
        def _(block):
            pj_copy(block, 1).wait_recv()

    pj_store = pltpu.make_async_copy(pj_all, pj_out, local_sem.at[1])
    pj_store.start()
    col_sketch = jnp.zeros((rank_dim, rank_dim), jnp.float32)
    for block in range(n_col):
        col_sketch += dot3_split(sk_both[block], pj_all[block], NT)

    left_core = dot3(col_sketch, gram, NN)
    nothing = jnp.zeros((rank_dim, 2 * rank_dim), jnp.bfloat16)

    def stacked(value):
        high, low = halves(value)
        return jnp.concatenate([
            jnp.concatenate([high, high], axis=1), jnp.concatenate([low, nothing], axis=1)
        ], axis=0)

    for slot in range(slots):
        lanes = slice(slot * rank_dim, (slot + 1) * rank_dim)
        right_core = dot3(row_sketch[:, lanes], gram[:, lanes], NT)
        y_left[slot] = stacked(
            jnp.concatenate([own_sketches[0, :, lanes], -left_core[:, lanes]], axis=1))
        z_left[slot] = stacked(
            jnp.concatenate([own_sketches[1, :, lanes], -right_core], axis=1))

    for step in range(1, n_col):
        loc_copy(col, step).wait_send()
        pend_copy(col, step).wait_send()
        g_copy(col, step).wait_send()
    for step in range(1, n_row):
        pv_copy(row, step).wait_send()
    for distance in range(n_z):
        @pl.when(z_pos + distance < n_z)
        def _(distance=distance):
            block = col + 2 * distance
            pu_copy(block, 2).wait_send()

            @pl.when(z_pos > 0)
            def _():
                pu_copy(block, 0).wait_send()

        @pl.when(z_pos - distance >= 0)
        def _(distance=distance):
            block = col - 2 * distance
            if distance:
                pu_copy(block, 2).wait_send()

            @pl.when(z_pos < n_z - 1)
            def _():
                pu_copy(block, 1).wait_send()

    @pl.when(is_owner)
    def _():
        @pl.loop(0, n_col)
        def _(block):
            for step in range(1, n_row):
                pj_copy(block, step).wait_send()

    pu_store.wait()
    pj_store.wait()


def finish(
    n_row, ranks, u_ref, v_ref, pu_ref, pj_ref, acc, y_left, z_left,
    trail_y, trail_z, pend_y, pend_z,
):
    row, col = lax.axis_index("row"), lax.axis_index("col")
    slots, rank_dim, w = u_ref.shape
    rank_iota = lax.broadcasted_iota(jnp.int32, (rank_dim, 1), 0)
    pj_high, pj_low = halves(pj_ref[0])

    def apply(left, first, second_high, second_low):
        high, low = halves(first)
        right = jnp.concatenate([high, second_high, low, second_low], axis=0)
        both = product(left, right, NN)
        return both[:rank_dim] + both[rank_dim:]

    for slot in range(slots):
        active = slot * n_row + row > col
        u_block = jnp.where(rank_iota < ranks[slot], u_ref[slot], 0.0)
        y_block = apply(y_left[slot], u_block, *halves(pu_ref[0, slot]))
        z_block = apply(z_left[slot], v_ref[slot], pj_high, pj_low)
        trail_y[slot, 0, 0] = jnp.where(active, y_block, 0.0)
        trail_z[slot, 0, 0] = jnp.where(active, z_block, 0.0)

    @pl.when(pl.program_id(0) == 0)
    def _():
        for slot in range(slots):
            lanes = slice(slot * w, (slot + 1) * w)
            pend_y[slot, 0] = acc[:, lanes] * matern_scale
            lanes = slice((slots + slot) * w, (slots + slot + 1) * w)
            pend_z[slot, 0] = acc[:, lanes] * matern_scale


def broadcast(block, axis, owner):
    block = jnp.where(lax.axis_index(axis) == owner, block, jnp.zeros_like(block))
    return lax.psum(block, axis)


def matmul(left, right):
    return jnp.dot(left, right, precision=lax.Precision.HIGHEST, preferred_element_type=jnp.float32)


def batched(form, left, right):
    return jnp.einsum(
        form, left, right, precision=lax.Precision.HIGHEST, preferred_element_type=jnp.float32
    )


def matern(row_points, col_points):
    delta_x = row_points[0][:, None] - col_points[0][None, :]
    delta_y = row_points[1][:, None] - col_points[1][None, :]
    distance = jnp.sqrt(delta_x * delta_x + delta_y * delta_y)
    scaled = root_three * distance / length_scale
    return matern_scale * (1.0 + scaled) * jnp.exp(-scaled)


def plain_on_device(trail_u, trail_v, ranks, panel_u, panel_v, locations, pend_locs, sketch):
    row_count = lax.axis_size("row")
    row_index = lax.axis_index("row")
    col_index = lax.axis_index("col")
    row_slots = trail_u.shape[0]
    rank_dim = trail_u.shape[3]
    width = trail_u.shape[4]
    local_width = pend_locs.shape[1]
    gathered_u, gathered_v = (
        lax.all_gather(panel_u, "col", axis=3, tiled=True),
        lax.all_gather(panel_v, "col", axis=3, tiled=True),
    )
    slot_index = col_index // row_count
    own_u = lax.dynamic_index_in_dim(gathered_u[:, 0], slot_index, 0, keepdims=False)
    own_v = lax.dynamic_index_in_dim(gathered_v[:, 0], slot_index, 0, keepdims=False)
    col_pu, col_pv = (
        broadcast(own_u, "row", col_index % row_count),
        broadcast(own_v, "row", col_index % row_count),
    )
    rank_iota = lax.broadcasted_iota(jnp.int32, (row_slots, rank_dim), 1)
    in_use = (rank_iota < ranks[:, 0, 0][:, None]).astype(jnp.float32)
    u_tiles = trail_u[:, 0, 0] * in_use[:, :, None]
    v_tiles = trail_v[:, 0, 0]
    row_pu = gathered_u[:, 0]
    row_pv = gathered_v[:, 0]
    v_sketch = batched("tkn,ln->tkl", v_tiles, sketch)
    u_sketch = batched("tkn,ln->tkl", u_tiles, sketch)
    cross_gram = batched("tkn,ln->tkl", row_pv, col_pv)
    col_sketch = matmul(col_pu, sketch.T)
    row_sketch = batched("tkn,ln->tkl", row_pu, sketch)
    left_core = batched("tkm,ml->tkl", cross_gram, col_sketch)
    y_tiles = batched("tkl,tkn->tln", v_sketch, u_tiles) - batched(
        "tkl,tkn->tln", left_core, row_pu
    )
    right_core = batched("tkl,tkm->tlm", row_sketch, cross_gram)
    z_tiles = batched("tkl,tkn->tln", u_sketch, v_tiles) - batched(
        "tlm,mn->tln", right_core, col_pu
    )
    tile_rows = jnp.arange(row_slots, dtype=jnp.int32) * row_count + row_index
    keep_mask = (tile_rows > col_index)[:, None, None]
    trail_y = jnp.where(keep_mask, y_tiles, 0.0).reshape(row_slots, 1, 1, rank_dim, width)
    trail_z = jnp.where(keep_mask, z_tiles, 0.0).reshape(row_slots, 1, 1, rank_dim, width)
    y_list = []
    z_list = []
    rows_all, pend_all = (
        lax.all_gather(locations, "col", axis=3, tiled=True),
        lax.all_gather(pend_locs.reshape(1, 1, 2, local_width), "col", axis=3, tiled=True),
    )
    col_points = pend_all[0, 0]
    for slot_num in range(row_slots):
        own_kernel = matern(locations[slot_num, 0], col_points)
        y_list.append(matmul(sketch, own_kernel.T))
        col_kernel = matern(rows_all[slot_num, 0], pend_locs)
        z_list.append(matmul(sketch, col_kernel))
    pend_y = jnp.stack(y_list)
    pend_z = jnp.stack(z_list)
    pend_y = pend_y.reshape(row_slots, 1, rank_dim, local_width)
    pend_z = pend_z.reshape(row_slots, 1, rank_dim, local_width)
    return (trail_y, trail_z, pend_y, pend_z)


def on_device(n_row, n_col, trail_u, trail_v, ranks, panel_u, panel_v, locations, pend_locs, sketch):
    slots, _, _, rank_dim, width = trail_u.shape
    w = pend_locs.shape[1]
    if w % 128 or rank_dim % 16 or n_col % 2:
        return plain_on_device(
            trail_u, trail_v, ranks, panel_u, panel_v, locations, pend_locs, sketch
        )
    flat = slots * rank_dim
    f32, bf16 = jnp.float32, jnp.bfloat16
    dma = pltpu.SemaphoreType.DMA
    vmem = pl.BlockSpec(memory_space=pltpu.VMEM)
    hbm = pl.BlockSpec(memory_space=pl.ANY)
    point_rows = -(-(2 * slots + 2) // 8) * 8
    ranks = ranks.reshape(slots)
    trail_u = trail_u.reshape(slots, rank_dim, width)
    trail_v = trail_v.reshape(slots, rank_dim, width)
    shape = jax.ShapeDtypeStruct
    smem = pl.BlockSpec(memory_space=pltpu.SMEM)
    pu_all, pj_all, acc, y_left, z_left = pl.pallas_call(
        functools.partial(kernel, n_row, n_col),
        out_shape=(
            shape((n_col, slots, rank_dim, w), f32),
            shape((n_col, rank_dim, w), f32),
            shape((rank_dim, 2 * slots * w), f32),
            shape((slots, 2 * rank_dim, 4 * rank_dim), bf16),
            shape((slots, 2 * rank_dim, 4 * rank_dim), bf16),
        ),
        in_specs=[smem, hbm, hbm] + [vmem] * 5,
        out_specs=(hbm, hbm, vmem, vmem, vmem),
        scratch_shapes=[
            pltpu.VMEM((slots, rank_dim, width), f32),
            pltpu.VMEM((slots, rank_dim, width), f32),
            pltpu.VMEM((n_col, slots, 2, w), f32),
            pltpu.VMEM((n_col, 2, w), f32),
            pltpu.VMEM((n_col, slots, rank_dim, w), f32),
            pltpu.VMEM((n_col, rank_dim, w), f32),
            pltpu.VMEM((n_row, slots, rank_dim, w), f32),
            pltpu.VMEM((n_col, rank_dim, flat), f32),
            pltpu.VMEM((n_col, rank_dim, flat), f32),
            pltpu.VMEM((1, w, point_rows), f32),
            pltpu.VMEM((2, 2 * slots * w), f32),
            pltpu.VMEM((n_col, 2 * rank_dim, w), bf16),
            pltpu.VMEM((w, 2 * slots * w), bf16),
            pltpu.VMEM((w, 2 * slots * w), bf16),
            pltpu.VMEM((2, rank_dim, flat), f32),
            dma((2,)),
            dma((n_col,)), dma((n_col,)), dma((n_col,)), dma((n_col,)),
            dma((3, n_col)), dma((n_col,)),
            dma((n_row, n_col)), dma((n_col,)),
            dma((n_row,)), dma((n_row,)),
            dma((n_col,)), dma((n_col,)),
        ],
        compiler_params=pltpu.CompilerParams(collective_id=0, has_side_effects=True),
    )(
        ranks,
        trail_u,
        trail_v,
        panel_u.reshape(slots, rank_dim, w),
        panel_v.reshape(slots, rank_dim, w),
        locations.reshape(slots, 2, w),
        pend_locs,
        sketch,
    )
    tile = pl.BlockSpec((slots, rank_dim, w), lambda block: (0, 0, block))
    out_tile = pl.BlockSpec((slots, 1, 1, rank_dim, w), lambda block: (0, 0, 0, 0, block))
    left = pl.BlockSpec((slots, 2 * rank_dim, 4 * rank_dim), lambda block: (0, 0, 0))
    pend_tile = pl.BlockSpec((slots, 1, rank_dim, w), lambda block: (0, 0, 0, 0))
    return pl.pallas_call(
        functools.partial(finish, n_row),
        grid=(n_col,),
        out_shape=(
            shape((slots, 1, 1, rank_dim, width), f32),
            shape((slots, 1, 1, rank_dim, width), f32),
            shape((slots, 1, rank_dim, w), f32),
            shape((slots, 1, rank_dim, w), f32),
        ),
        in_specs=[
            smem, tile, tile,
            pl.BlockSpec((1, slots, rank_dim, w), lambda block: (block, 0, 0, 0)),
            pl.BlockSpec((1, rank_dim, w), lambda block: (block, 0, 0)),
            pl.BlockSpec((rank_dim, 2 * slots * w), lambda block: (0, 0)),
            left, left,
        ],
        out_specs=(out_tile, out_tile, pend_tile, pend_tile),
    )(ranks, trail_u, trail_v, pu_all, pj_all, acc, y_left, z_left)


def solution(mesh):
    in_specs = (
        P(None, "row", "col", None, None),
        P(None, "row", "col", None, None),
        P(None, "row", "col"),
        P(None, "row", None, "col"),
        P(None, "row", None, "col"),
        P(None, "row", None, "col"),
        P(None, "col"),
        P(),
    )
    out_specs = (
        P(None, "row", "col", None, None),
        P(None, "row", "col", None, None),
        P(None, "row", None, "col"),
        P(None, "row", None, "col"),
    )
    body = functools.partial(on_device, mesh.shape["row"], mesh.shape["col"])
    return jax.shard_map(
        body, mesh=mesh, in_specs=in_specs, out_specs=out_specs, check_vma=False
    )
```
